32 devices in a mesh: lat: 16 (over z, x, core), lon: 2 (over y).
Axes of the slice: x: 2, y: 2, z: 4, core: 2. Of those that a mesh axis runs over, the one named last changes fastest.
Arguments:
- elevation: float32 [4096, 4096], P('lat', 'lon'), may hold values from -200 to 200
Outputs:
- slope_angle: float32 [4096, 4096], P('lat', 'lon')
- facing: float32 [2, 4096, 4096], P(None, 'lat', 'lon')
- hillshade: float32 [4096, 4096], P('lat', 'lon')
The draws below stay inside these ranges and needn't reach their ends.
All inputs are finite; a program needn't handle non-finite values.
Results may differ from the reference program's by a relative error of at most 0.0003.
Values sent between devices are 32-bit elements; how exact they have to be, the bound alone decides.
A program may use at most 64 MiB of HBM per device.

```python
import math
import jax
import jax.numpy as jnp
from jax import lax

SCALES = 7
HALO = 64
NROWS = 4096
NCOLS = 4096


def draw_elevation(key, part):
    surface = jnp.zeros((NROWS, NCOLS), jnp.float32)
    for octave in range(SCALES):
        stride = 2 ** octave
        noise_key = jax.random.fold_in(key, 11 + octave)
        shift_key = jax.random.fold_in(key, 101 + octave)
        coarse_shape = (NROWS // stride, NCOLS // stride)
        coarse = jax.random.truncated_normal(noise_key, -4.0, 4.0, coarse_shape, jnp.float32)
        amplitude = 2.0 * math.sqrt(stride)
        upsampled = jnp.repeat(jnp.repeat(coarse, stride, axis=0), stride, axis=1)
        offsets = jax.random.randint(shift_key, (2,), 0, stride)
        upsampled = jnp.roll(upsampled, (offsets[0], offsets[1]), axis=(0, 1))
        surface = surface + amplitude * upsampled
    return surface


def setup_inputs(seed: int = 0) -> dict:
    streams_of = jax.random.split(jax.random.key(seed), 2)
    elevation = draw_elevation(jax.random.fold_in(streams_of[1], 71), 0)
    return dict(elevation=elevation)


LIGHT_EAST = -0.5
LIGHT_NORTH = 0.5
LIGHT_UP = math.sqrt(0.5)

def window(padded, margin, row_offset, col_offset, row_count, col_count):
    return lax.slice(padded, (margin + row_offset, margin + col_offset), (margin + row_offset + row_count, margin + col_offset + col_count))

def terrain_shading(padded, spacing, margin, levels):
    row_count = padded.shape[0] - 2 * margin
    col_count = padded.shape[1] - 2 * margin
    eastward = jnp.zeros((row_count, col_count), jnp.float32)
    northward = jnp.zeros((row_count, col_count), jnp.float32)
    for octave in range(levels):
        stride = 2 ** octave
        north_west = window(padded, margin, -stride, -stride, row_count, col_count)
        north_mid = window(padded, margin, -stride, 0, row_count, col_count)
        north_east = window(padded, margin, -stride, stride, row_count, col_count)
        west_mid = window(padded, margin, 0, -stride, row_count, col_count)
        east_mid = window(padded, margin, 0, stride, row_count, col_count)
        south_west = window(padded, margin, stride, -stride, row_count, col_count)
        south_mid = window(padded, margin, stride, 0, row_count, col_count)
        south_east = window(padded, margin, stride, stride, row_count, col_count)
        east_diff = north_east + 2.0 * east_mid + south_east - (north_west + 2.0 * west_mid + south_west)
        north_diff = north_west + 2.0 * north_mid + north_east - (south_west + 2.0 * south_mid + south_east)
        eastward = eastward + east_diff * (1.0 / stride)
        northward = northward + north_diff * (1.0 / stride)
    grad_east = eastward / (8.0 * levels * spacing[:, None])
    grad_north = northward * (1.0 / (8.0 * levels))
    squared = grad_east * grad_east + grad_north * grad_north
    slope_angle = jnp.arctan(jnp.sqrt(squared))
    inverse = lax.rsqrt(1.0 + squared)
    facing_east = -grad_east * inverse
    facing_north = -grad_north * inverse
    shading = jnp.maximum(LIGHT_EAST * facing_east + LIGHT_NORTH * facing_north + LIGHT_UP * inverse, 0.0)
    return (slope_angle, jnp.stack([facing_east, facing_north]), shading)

def reference(elevation):
    margin = HALO
    wrapped = jnp.concatenate([elevation[:, NCOLS - margin:], elevation, elevation[:, :margin]], axis=1)
    padded = jnp.concatenate([jnp.broadcast_to(wrapped[:1], (margin, NCOLS + 2 * margin)), wrapped, jnp.broadcast_to(wrapped[NROWS - 1:], (margin, NCOLS + 2 * margin))], axis=0)
    position = jnp.arange(NROWS, dtype=jnp.int32)
    spacing = jnp.sin((position.astype(jnp.float32) + 0.5) * (math.pi / NROWS)) * (2.0 * NROWS / NCOLS)
    block_rows = math.gcd(NROWS, 512)
    block_count = NROWS // block_rows

    def one_block(number):
        first_row = (number * block_rows).astype(jnp.int32)
        slab = lax.dynamic_slice(padded, (first_row, jnp.int32(0)), (block_rows + 2 * margin, NCOLS + 2 * margin))
        slab_spacing = lax.dynamic_slice(spacing, (first_row,), (block_rows,))
        return terrain_shading(slab, slab_spacing, margin, SCALES)
    results = lax.map(one_block, jnp.arange(block_count, dtype=jnp.int32))
    slope_angle = results[0].reshape(NROWS, NCOLS)
    facing = jnp.transpose(results[1], (1, 0, 2, 3)).reshape(2, NROWS, NCOLS)
    hillshade = results[2].reshape(NROWS, NCOLS)
    return (slope_angle, facing, hillshade)
```

```python
import functools
import math

import jax
import jax.numpy as jnp
from jax import lax
from jax.experimental import pallas as pl
from jax.experimental.pallas import tpu as pltpu
from jax.sharding import PartitionSpec as P

SCALES = 7
HALO = 64
LANES = 128
SUB = 8
GROUP = 4

LIGHT_UP = math.sqrt(0.5)
MESH = pl.DeviceIdType.MESH

ANGLE = (
    1.5707963068901982,
    -0.9999960003074525,
    0.7852630240552405,
    -0.6648577772093989,
    0.5764135907397322,
    -0.48061340102986794,
    0.3483872625788081,
    -0.19210392123613929,
    0.06787372952021542,
    -0.011162824266648386,
)


def row_pad(stride):
    return max(stride, SUB)


def kernel(rows, cols, z_ref, coef_ref, slope_ref, facing_ref, shade_ref, *scratch):
    lags, (zbuf, wsum, load_sem, send_sem, recv_sem, rim_send, rim_recv) = (
        scratch[:SCALES],
        scratch[SCALES:],
    )
    lat, lon = lax.axis_index("lat"), lax.axis_index("lon")
    n_lat, n_lon = lax.axis_size("lat"), lax.axis_size("lon")
    west, east = lax.rem(lon + n_lon - 1, n_lon), lax.rem(lon + 1, n_lon)
    strips = cols // LANES
    groups = strips // GROUP
    exists = (lat > 0, lat < n_lat - 1)
    neighbour = (lat - 1, lat + 1)
    lane = lax.broadcasted_iota(jnp.int32, (SUB, LANES), 1)

    edge_rows = (0, rows - HALO)
    loads = []
    for number, (start, count) in enumerate(
        ((0, HALO), (rows - HALO, HALO), (HALO, rows - 2 * HALO))
    ):
        load = pltpu.make_async_copy(
            z_ref.at[pl.ds(start, count), :],
            zbuf.at[pl.ds(HALO + start, count), pl.ds(LANES, cols)],
            load_sem.at[number],
        )
        load.start()
        loads.append(load)

    barrier = pltpu.get_barrier_semaphore()
    for side_lon in (west, east):
        pl.semaphore_signal(barrier, inc=1, device_id=(lat, side_lon), device_id_type=MESH)
    for side in range(2):

        @pl.when(exists[side])
        def _():
            for other in (lon, west, east):
                pl.semaphore_signal(
                    barrier, inc=1, device_id=(neighbour[side], other), device_id_type=MESH
                )

    pl.semaphore_wait(
        barrier, 2 + 3 * (exists[0].astype(jnp.int32) + exists[1].astype(jnp.int32))
    )

    bounds = [0] + [min(GROUP * k + 1, strips) for k in range(1, groups)] + [strips]

    def piece(number):
        if number == groups:
            return 0, LANES
        if number == groups + 1:
            return LANES + cols, LANES
        return LANES + bounds[number] * LANES, (bounds[number + 1] - bounds[number]) * LANES

    def lat_copy(side, number):
        start, width = piece(number)
        source_start, other = start, lon
        if number == groups:
            source_start, start, other = LANES, LANES + cols, west
        if number == groups + 1:
            source_start, start, other = cols, 0, east
        index = number
        if number == groups:
            index = groups + 1
        if number == groups + 1:
            index = groups
        target_row = HALO + rows if side == 0 else 0
        return pltpu.make_async_remote_copy(
            src_ref=zbuf.at[pl.ds(HALO + edge_rows[side], HALO), pl.ds(source_start, width)],
            dst_ref=zbuf.at[pl.ds(target_row, HALO), pl.ds(start, width)],
            send_sem=send_sem.at[side, number],
            recv_sem=recv_sem.at[1 - side, index],
            device_id=(neighbour[side], other),
            device_id_type=MESH,
        )

    def rim_copy(side):
        source_start, start, other = ((LANES, LANES + cols, west), (cols, 0, east))[side]
        return pltpu.make_async_remote_copy(
            src_ref=zbuf.at[pl.ds(HALO, rows), pl.ds(source_start, LANES)],
            dst_ref=zbuf.at[pl.ds(HALO, rows), pl.ds(start, LANES)],
            send_sem=rim_send.at[side],
            recv_sem=rim_recv.at[side],
            device_id=(lat, other),
            device_id_type=MESH,
        )

    order = [groups + 1] + list(range(groups)) + [groups]
    for side in range(2):
        loads[side].wait()

        @pl.when(exists[side])
        def _():
            for number in order:
                lat_copy(side, number).start()

    loads[2].wait()
    for side in range(2):
        rim_copy(side).start()

    def widen(first_row, count, octaves, group, with_centre):
        def step(index, carry):
            row = pl.multiple_of(first_row + index * SUB, SUB)
            column = pl.multiple_of(group * (GROUP * LANES), LANES)
            z = [
                zbuf[pl.ds(row, SUB), pl.ds(column + k * LANES, LANES)] for k in range(GROUP + 2)
            ]
            centre = [None] * GROUP
            for octave in octaves:
                stride = 2**octave
                scaled = [v * (1.0 / stride) for v in z] if octave else z
                ahead = [pltpu.roll(v, LANES - stride, 1) for v in scaled[1:]]
                if 2 * stride == LANES:
                    behind = [pltpu.roll(scaled[0], stride, 1)] + ahead[:-1]
                else:
                    behind = [pltpu.roll(v, stride, 1) for v in scaled[:-1]]
                store_row = pl.multiple_of(row - HALO + row_pad(stride), SUB)
                for k in range(GROUP):
                    plus = jnp.where(lane < LANES - stride, ahead[k], ahead[k + 1])
                    minus = jnp.where(lane >= stride, behind[k + 1], behind[k])
                    strip = group * GROUP + k
                    lags[octave][0, strip, pl.ds(store_row, SUB), :] = scaled[k + 1] + plus
                    lags[octave][1, strip, pl.ds(store_row, SUB), :] = scaled[k + 1] + minus
                    if with_centre:
                        term = plus - minus
                        centre[k] = term if centre[k] is None else centre[k] + term
            if with_centre:
                for k in range(GROUP):
                    wsum[group * GROUP + k, pl.ds(pl.multiple_of(row - HALO, SUB), SUB), :] = (
                        centre[k] + centre[k]
                    )
            return carry

        lax.fori_loop(0, count // SUB, step, 0)

    def shade(first_row, count, group):
        def step(index, carry):
            row = pl.multiple_of(first_row + index * SUB, SUB)
            coef = coef_ref[pl.ds(row, SUB), :]
            for k in range(GROUP):
                strip = group * GROUP + k
                down = up = None
                for octave in range(SCALES):
                    stride = 2**octave
                    lag = lags[octave]
                    north = pl.ds(row + (row_pad(stride) - stride), SUB)
                    south = pl.ds(row + (row_pad(stride) + stride), SUB)
                    a = lag[0, strip, south, :] - lag[1, strip, north, :]
                    b = lag[0, strip, north, :] - lag[1, strip, south, :]
                    down = a if down is None else down + a
                    up = b if up is None else up + b
                grad_east = (wsum[strip, pl.ds(row, SUB), :] + (down + up)) * coef
                grad_north = (up - down) * (1.0 / (8.0 * SCALES))
                squared = grad_east * grad_east + grad_north * grad_north
                inverse = lax.rsqrt(1.0 + squared)
                sine = squared * lax.rsqrt(jnp.maximum(squared, 1e-37)) * inverse
                ratio = jnp.full_like(inverse, ANGLE[-1])
                for term in ANGLE[-2::-1]:
                    ratio = ratio * inverse + term
                facing_east = -grad_east * inverse
                facing_north = -grad_north * inverse
                shading = jnp.maximum(
                    0.5 * (facing_north - facing_east) + LIGHT_UP * inverse, 0.0
                )
                place = (
                    pl.ds(row, SUB),
                    pl.ds(pl.multiple_of(group * (GROUP * LANES), LANES) + k * LANES, LANES),
                )
                slope_ref[place] = sine * ratio
                facing_ref[(0,) + place] = facing_east
                facing_ref[(1,) + place] = facing_north
                shade_ref[place] = shading
            return carry

        lax.fori_loop(0, count // SUB, step, 0)

    def inner(index, carry):
        group = lax.rem(index + 1, groups)

        @pl.when(index == max(groups - 2, 0))
        def _():
            for side in range(2):
                rim_copy(side).wait_recv()

        widen(HALO, rows, range(SCALES), group, True)
        shade(HALO, rows - 2 * HALO, group)
        return carry

    lax.fori_loop(0, groups, inner, 0)

    near = 1 - lax.rem(lat, 2)

    def outer(index, carry):
        side = jnp.where(index == 0, near, 1 - near)
        here = jnp.where(side == 0, lat > 0, lat < n_lat - 1)
        top = side == 0
        halo_row = pl.multiple_of(jnp.where(top, 0, HALO + rows), SUB)

        def wait_piece(number):
            start, width = piece(number)
            pltpu.make_async_remote_copy(
                src_ref=zbuf.at[pl.ds(halo_row, HALO), pl.ds(start, width)],
                dst_ref=zbuf.at[pl.ds(halo_row, HALO), pl.ds(start, width)],
                send_sem=send_sem.at[0, number],
                recv_sem=recv_sem.at[side, number],
                device_id=(lat, east),
                device_id_type=MESH,
            ).wait_recv()

        for pole in range(2):

            @pl.when(jnp.logical_and(jnp.logical_not(here), side == pole))
            def _():
                first = HALO if pole == 0 else HALO + rows - SUB
                pick = 0 if pole == 0 else SUB - 1
                fill = 0 if pole == 0 else HALO + rows

                def repeat(strip, carry):
                    column = pl.ds(pl.multiple_of(strip * LANES, LANES), LANES)
                    edge = zbuf[pl.ds(first, SUB), column][pick : pick + 1]
                    block = jnp.broadcast_to(edge, (SUB, LANES))
                    for k in range(HALO // SUB):
                        zbuf[pl.ds(fill + k * SUB, SUB), column] = block
                    return carry

                lax.fori_loop(0, strips + 2, repeat, 0)

        def one_group(group, carry):
            for k in range(groups):

                @pl.when(jnp.logical_and(here, group == k))
                def _():
                    wait_piece(k)
                    if k == 0:
                        wait_piece(groups)
                    if k == groups - 1:
                        wait_piece(groups + 1)

            reach = 0
            for octave in range(SCALES):
                stride = 2**octave
                if stride < SUB:
                    continue
                first = jnp.where(top, HALO - stride, HALO + rows + reach)
                octaves = range(SCALES) if reach == 0 else range(octave, SCALES)
                widen(first, stride - reach, octaves, group, False)
                reach = stride
            shade(jnp.where(top, 0, rows - HALO), HALO, group)
            return carry

        lax.fori_loop(0, groups, one_group, 0)
        return carry

    lax.fori_loop(0, 2, outer, 0)

    for side in range(2):
        rim_copy(side).wait_send()

        @pl.when(exists[side])
        def _():
            for number in order:
                lat_copy(side, number).wait_send()


def local(elevation):
    rows, cols = elevation.shape
    strips = cols // LANES
    groups = strips // GROUP
    total_rows = rows * lax.axis_size("lat")
    total_cols = cols * lax.axis_size("lon")
    position = lax.axis_index("lat") * rows + lax.iota(jnp.int32, rows)
    spacing = jnp.sin((position.astype(jnp.float32) + 0.5) * (math.pi / total_rows)) * (
        2.0 * total_rows / total_cols
    )
    coef = jnp.broadcast_to((1.0 / (8.0 * SCALES * spacing))[:, None], (rows, LANES))
    return tuple(
        pl.pallas_call(
            functools.partial(kernel, rows, cols),
            out_shape=(
                pltpu.VMEM((rows, cols), jnp.float32),
                pltpu.VMEM((2, rows, cols), jnp.float32),
                pltpu.VMEM((rows, cols), jnp.float32),
            ),
            in_specs=[
                pl.BlockSpec(memory_space=pl.ANY),
                pl.BlockSpec(memory_space=pltpu.VMEM),
            ],
            out_specs=tuple([pl.BlockSpec(memory_space=pltpu.VMEM)] * 3),
            scratch_shapes=[
                pltpu.VMEM((2, strips, rows + 2 * row_pad(2**k), LANES), jnp.float32)
                for k in range(SCALES)
            ]
            + [
                pltpu.VMEM((rows + 2 * HALO, cols + 2 * LANES), jnp.float32),
                pltpu.VMEM((strips, rows, LANES), jnp.float32),
                pltpu.SemaphoreType.DMA((3,)),
                pltpu.SemaphoreType.DMA((2, groups + 2)),
                pltpu.SemaphoreType.DMA((2, groups + 2)),
                pltpu.SemaphoreType.DMA((2,)),
                pltpu.SemaphoreType.DMA((2,)),
            ],
            compiler_params=pltpu.CompilerParams(
                collective_id=0, has_side_effects=True, vmem_limit_bytes=52 * 2**20
            ),
        )(elevation, coef)
    )


def solution(mesh):
    in_specs = (P("lat", "lon"),)
    out_specs = (P("lat", "lon"), P(None, "lat", "lon"), P("lat", "lon"))
    return jax.shard_map(local, mesh=mesh, in_specs=in_specs, out_specs=out_specs, check_vma=False)
```

```python
import functools
import math

import jax
import jax.numpy as jnp
from jax import lax
from jax.experimental import pallas as pl
from jax.experimental.pallas import tpu as pltpu
from jax.sharding import PartitionSpec as P

SCALES = 7
HALO = 64
LANES = 128
SUB = 8
GROUP = 8

LIGHT_UP = math.sqrt(0.5)
MESH = pl.DeviceIdType.MESH

ANGLE = (
    1.5707963068901982,
    -0.9999960003074525,
    0.7852630240552405,
    -0.6648577772093989,
    0.5764135907397322,
    -0.48061340102986794,
    0.3483872625788081,
    -0.19210392123613929,
    0.06787372952021542,
    -0.011162824266648386,
)


def row_pad(stride):
    return max(stride, SUB)


def kernel(rows, cols, z_ref, coef_ref, slope_ref, facing_ref, shade_ref, *scratch):
    lags, (zbuf, wsum, load_sem, send_sem, recv_sem, rim_send, rim_recv) = (
        scratch[:SCALES],
        scratch[SCALES:],
    )
    lat, lon = lax.axis_index("lat"), lax.axis_index("lon")
    n_lat, n_lon = lax.axis_size("lat"), lax.axis_size("lon")
    west, east = lax.rem(lon + n_lon - 1, n_lon), lax.rem(lon + 1, n_lon)
    strips = cols // LANES
    groups = strips // GROUP
    exists = (lat > 0, lat < n_lat - 1)
    neighbour = (lat - 1, lat + 1)
    lane = lax.broadcasted_iota(jnp.int32, (SUB, LANES), 1)

    edge_rows = (0, rows - HALO)
    loads = []
    for number, (start, count) in enumerate(
        ((0, HALO), (rows - HALO, HALO), (HALO, rows - 2 * HALO))
    ):
        load = pltpu.make_async_copy(
            z_ref.at[pl.ds(start, count), :],
            zbuf.at[pl.ds(HALO + start, count), pl.ds(LANES, cols)],
            load_sem.at[number],
        )
        load.start()
        loads.append(load)

    barrier = pltpu.get_barrier_semaphore()
    for side_lon in (west, east):
        pl.semaphore_signal(barrier, inc=1, device_id=(lat, side_lon), device_id_type=MESH)
    for side in range(2):

        @pl.when(exists[side])
        def _():
            for other in (lon, west, east):
                pl.semaphore_signal(
                    barrier, inc=1, device_id=(neighbour[side], other), device_id_type=MESH
                )

    pl.semaphore_wait(
        barrier, 2 + 3 * (exists[0].astype(jnp.int32) + exists[1].astype(jnp.int32))
    )

    bounds = [0] + [min(GROUP * k + 1, strips) for k in range(1, groups)] + [strips]

    def piece(number):
        if number == groups:
            return 0, LANES
        if number == groups + 1:
            return LANES + cols, LANES
        return LANES + bounds[number] * LANES, (bounds[number + 1] - bounds[number]) * LANES

    def lat_copy(side, number):
        start, width = piece(number)
        source_start, other = start, lon
        if number == groups:
            source_start, start, other = LANES, LANES + cols, west
        if number == groups + 1:
            source_start, start, other = cols, 0, east
        index = number
        if number == groups:
            index = groups + 1
        if number == groups + 1:
            index = groups
        target_row = HALO + rows if side == 0 else 0
        return pltpu.make_async_remote_copy(
            src_ref=zbuf.at[pl.ds(HALO + edge_rows[side], HALO), pl.ds(source_start, width)],
            dst_ref=zbuf.at[pl.ds(target_row, HALO), pl.ds(start, width)],
            send_sem=send_sem.at[side, number],
            recv_sem=recv_sem.at[1 - side, index],
            device_id=(neighbour[side], other),
            device_id_type=MESH,
        )

    def rim_copy(side):
        source_start, start, other = ((LANES, LANES + cols, west), (cols, 0, east))[side]
        return pltpu.make_async_remote_copy(
            src_ref=zbuf.at[pl.ds(HALO, rows), pl.ds(source_start, LANES)],
            dst_ref=zbuf.at[pl.ds(HALO, rows), pl.ds(start, LANES)],
            send_sem=rim_send.at[side],
            recv_sem=rim_recv.at[side],
            device_id=(lat, other),
            device_id_type=MESH,
        )

    order = [groups + 1] + list(range(groups)) + [groups]
    for side in range(2):
        loads[side].wait()

        @pl.when(exists[side])
        def _():
            for number in order:
                lat_copy(side, number).start()

    loads[2].wait()
    for side in range(2):
        rim_copy(side).start()

    def column_of(group):
        return pl.multiple_of(group * (GROUP * LANES), LANES)

    def rotate(row, octaves, group):
        column = column_of(group)
        z = [zbuf[pl.ds(row, SUB), pl.ds(column + k * LANES, LANES)] for k in range(GROUP + 2)]
        found = []
        for octave in octaves:
            stride = 2**octave
            scaled = [v * (1.0 / stride) for v in z] if octave else z
            ahead = [pltpu.roll(v, LANES - stride, 1) for v in scaled[1:]]
            if 2 * stride == LANES:
                behind = [pltpu.roll(scaled[0], stride, 1)] + ahead[:-1]
            else:
                behind = [pltpu.roll(v, stride, 1) for v in scaled[:-1]]
            found.append((octave, scaled, ahead, behind))
        return found

    def store(row, found, group, with_centre):
        centre = [None] * GROUP
        for octave, scaled, ahead, behind in found:
            stride = 2**octave
            store_row = pl.multiple_of(row - HALO + row_pad(stride), SUB)
            for k in range(GROUP):
                plus = jnp.where(lane < LANES - stride, ahead[k], ahead[k + 1])
                minus = jnp.where(lane >= stride, behind[k + 1], behind[k])
                strip = group * GROUP + k
                lags[octave][0, strip, pl.ds(store_row, SUB), :] = scaled[k + 1] + plus
                lags[octave][1, strip, pl.ds(store_row, SUB), :] = scaled[k + 1] + minus
                if with_centre:
                    term = plus - minus
                    centre[k] = term if centre[k] is None else centre[k] + term
        if with_centre:
            for k in range(GROUP):
                wsum[group * GROUP + k, pl.ds(pl.multiple_of(row - HALO, SUB), SUB), :] = (
                    centre[k] + centre[k]
                )

    def shade(row, group):
        coef = coef_ref[pl.ds(row, SUB), :]
        for k in range(GROUP):
            strip = group * GROUP + k
            down = up = None
            for octave in range(SCALES):
                stride = 2**octave
                lag = lags[octave]
                north = pl.ds(row + (row_pad(stride) - stride), SUB)
                south = pl.ds(row + (row_pad(stride) + stride), SUB)
                a = lag[0, strip, south, :] - lag[1, strip, north, :]
                b = lag[0, strip, north, :] - lag[1, strip, south, :]
                down = a if down is None else down + a
                up = b if up is None else up + b
            grad_east = (wsum[strip, pl.ds(row, SUB), :] + (down + up)) * coef
            grad_north = (up - down) * (1.0 / (8.0 * SCALES))
            squared = grad_east * grad_east + grad_north * grad_north
            inverse = lax.rsqrt(1.0 + squared)
            sine = squared * lax.rsqrt(jnp.maximum(squared, 1e-37)) * inverse
            ratio = jnp.full_like(inverse, ANGLE[-1])
            for term in ANGLE[-2::-1]:
                ratio = ratio * inverse + term
            facing_east = -grad_east * inverse
            facing_north = -grad_north * inverse
            shading = jnp.maximum(0.5 * (facing_north - facing_east) + LIGHT_UP * inverse, 0.0)
            place = (pl.ds(row, SUB), pl.ds(column_of(group) + k * LANES, LANES))
            slope_ref[place] = sine * ratio
            facing_ref[(0,) + place] = facing_east
            facing_ref[(1,) + place] = facing_north
            shade_ref[place] = shading

    near = 1 - lax.rem(lat, 2)
    far = 1 - near
    near_top = near == 0
    far_exists = jnp.where(near_top, exists[1], exists[0])

    def row_at(step):
        return pl.multiple_of(jnp.where(near_top, step * SUB, rows - SUB - step * SUB), SUB)

    def halo_row(side):
        return pl.multiple_of(jnp.where(side == 0, 0, HALO + rows), SUB)

    def wait_piece(side, number):
        start, width = piece(number)
        here = zbuf.at[pl.ds(halo_row(side), HALO), pl.ds(start, width)]
        pltpu.make_async_remote_copy(
            src_ref=here,
            dst_ref=here,
            send_sem=send_sem.at[0, number],
            recv_sem=recv_sem.at[side, number],
            device_id=(lat, east),
            device_id_type=MESH,
        ).wait_recv()

    def widen_halo(side, group):
        for distance in range(0, HALO, SUB):
            row = pl.multiple_of(
                jnp.where(side == 0, HALO - SUB - distance, HALO + rows + distance), SUB
            )
            octaves = [k for k in range(SCALES) if row_pad(2**k) > distance]
            store(row, rotate(row, octaves, group), group, False)

    ahead_steps = HALO // SUB + 1
    steps = rows // SUB

    def inner(index, carry):
        group = lax.rem(index + 1, groups)

        @pl.when(index == max(groups - 2, 0))
        def _():
            for side in range(2):
                rim_copy(side).wait_recv()

        def alone(step, carry):
            row = row_at(step) + HALO
            store(row, rotate(row, range(SCALES), group), group, True)
            return carry

        lax.fori_loop(0, ahead_steps, alone, 0)

        @pl.when(index == 0)
        def _():
            for number in order:
                wait_piece(near, number)

        widen_halo(near, group)

        def both(step, carry):
            row = row_at(step + ahead_steps) + HALO
            found = rotate(row, range(SCALES), group)
            shade(row_at(step), group)
            store(row, found, group, True)
            return carry

        lax.fori_loop(0, steps - ahead_steps, both, 0)
        return carry

    lax.fori_loop(0, groups, inner, 0)

    for pole in range(2):

        @pl.when(jnp.logical_and(jnp.logical_not(far_exists), far == pole))
        def _():
            first = HALO if pole == 0 else HALO + rows - SUB
            pick = 0 if pole == 0 else SUB - 1
            fill = 0 if pole == 0 else HALO + rows

            def repeat(strip, carry):
                column = pl.ds(pl.multiple_of(strip * LANES, LANES), LANES)
                edge = zbuf[pl.ds(first, SUB), column][pick : pick + 1]
                block = jnp.broadcast_to(edge, (SUB, LANES))
                for k in range(HALO // SUB):
                    zbuf[pl.ds(fill + k * SUB, SUB), column] = block
                return carry

            lax.fori_loop(0, strips + 2, repeat, 0)

    def last(group, carry):
        for k in range(groups):

            @pl.when(jnp.logical_and(far_exists, group == k))
            def _():
                wait_piece(far, k)
                if k == 0:
                    wait_piece(far, groups)
                if k == groups - 1:
                    wait_piece(far, groups + 1)

        widen_halo(far, group)

        def finish(step, carry):
            shade(row_at(step + steps - ahead_steps), group)
            return carry

        lax.fori_loop(0, ahead_steps, finish, 0)
        return carry

    lax.fori_loop(0, groups, last, 0)

    for side in range(2):
        rim_copy(side).wait_send()

        @pl.when(exists[side])
        def _():
            for number in order:
                lat_copy(side, number).wait_send()


def local(elevation):
    rows, cols = elevation.shape
    strips = cols // LANES
    groups = strips // GROUP
    total_rows = rows * lax.axis_size("lat")
    total_cols = cols * lax.axis_size("lon")
    position = lax.axis_index("lat") * rows + lax.iota(jnp.int32, rows)
    spacing = jnp.sin((position.astype(jnp.float32) + 0.5) * (math.pi / total_rows)) * (
        2.0 * total_rows / total_cols
    )
    coef = jnp.broadcast_to((1.0 / (8.0 * SCALES * spacing))[:, None], (rows, LANES))
    return tuple(
        pl.pallas_call(
            functools.partial(kernel, rows, cols),
            out_shape=(
                pltpu.VMEM((rows, cols), jnp.float32),
                pltpu.VMEM((2, rows, cols), jnp.float32),
                pltpu.VMEM((rows, cols), jnp.float32),
            ),
            in_specs=[
                pl.BlockSpec(memory_space=pl.ANY),
                pl.BlockSpec(memory_space=pltpu.VMEM),
            ],
            out_specs=tuple([pl.BlockSpec(memory_space=pltpu.VMEM)] * 3),
            scratch_shapes=[
                pltpu.VMEM((2, strips, rows + 2 * row_pad(2**k), LANES), jnp.float32)
                for k in range(SCALES)
            ]
            + [
                pltpu.VMEM((rows + 2 * HALO, cols + 2 * LANES), jnp.float32),
                pltpu.VMEM((strips, rows, LANES), jnp.float32),
                pltpu.SemaphoreType.DMA((3,)),
                pltpu.SemaphoreType.DMA((2, groups + 2)),
                pltpu.SemaphoreType.DMA((2, groups + 2)),
                pltpu.SemaphoreType.DMA((2,)),
                pltpu.SemaphoreType.DMA((2,)),
            ],
            compiler_params=pltpu.CompilerParams(
                collective_id=0, has_side_effects=True, vmem_limit_bytes=52 * 2**20
            ),
        )(elevation, coef)
    )


def solution(mesh):
    in_specs = (P("lat", "lon"),)
    out_specs = (P("lat", "lon"), P(None, "lat", "lon"), P("lat", "lon"))
    return jax.shard_map(local, mesh=mesh, in_specs=in_specs, out_specs=out_specs, check_vma=False)
```

```python
import functools
import math

import jax
import jax.numpy as jnp
from jax import lax
from jax.experimental import pallas as pl
from jax.experimental.pallas import tpu as pltpu
from jax.sharding import PartitionSpec as P

SCALES = 7
HALO = 64
LANES = 128
SUB = 8
GROUP = 8

LIGHT_UP = math.sqrt(0.5)
MESH = pl.DeviceIdType.MESH

ANGLE = (
    1.5707963068901982,
    -0.9999960003074525,
    0.7852630240552405,
    -0.6648577772093989,
    0.5764135907397322,
    -0.48061340102986794,
    0.3483872625788081,
    -0.19210392123613929,
    0.06787372952021542,
    -0.011162824266648386,
)


def row_pad(stride):
    return max(stride, SUB)


def kernel(rows, cols, z_ref, slope_ref, facing_ref, shade_ref, *scratch):
    lags, (zbuf, wsum, coef_ref, load_sem, send_sem, recv_sem, rim_send, rim_recv) = (
        scratch[:SCALES],
        scratch[SCALES:],
    )
    lat, lon = lax.axis_index("lat"), lax.axis_index("lon")
    n_lat, n_lon = lax.axis_size("lat"), lax.axis_size("lon")
    west, east = lax.rem(lon + n_lon - 1, n_lon), lax.rem(lon + 1, n_lon)
    strips = cols // LANES
    groups = strips // GROUP
    exists = (lat > 0, lat < n_lat - 1)
    neighbour = (lat - 1, lat + 1)
    lane = lax.broadcasted_iota(jnp.int32, (SUB, LANES), 1)

    edge_rows = (0, rows - HALO)
    loads = []
    for number, (start, count) in enumerate(
        ((0, HALO), (rows - HALO, HALO), (HALO, rows - 2 * HALO))
    ):
        load = pltpu.make_async_copy(
            z_ref.at[pl.ds(start, count), :],
            zbuf.at[pl.ds(HALO + start, count), pl.ds(LANES, cols)],
            load_sem.at[number],
        )
        load.start()
        loads.append(load)

    barrier = pltpu.get_barrier_semaphore()
    for side_lon in (west, east):
        pl.semaphore_signal(barrier, inc=1, device_id=(lat, side_lon), device_id_type=MESH)
    for side in range(2):

        @pl.when(exists[side])
        def _():
            for other in (lon, west, east):
                pl.semaphore_signal(
                    barrier, inc=1, device_id=(neighbour[side], other), device_id_type=MESH
                )

    total_rows = rows * n_lat
    total_cols = cols * n_lon
    for start in range(0, rows, SUB):
        position = lat * rows + start + lax.broadcasted_iota(jnp.int32, (SUB, LANES), 0)
        spacing = jnp.sin((position.astype(jnp.float32) + 0.5) * (math.pi / total_rows)) * (
            2.0 * total_rows / total_cols
        )
        coef_ref[pl.ds(start, SUB), :] = 1.0 / (8.0 * SCALES * spacing)

    pl.semaphore_wait(
        barrier, 2 + 3 * (exists[0].astype(jnp.int32) + exists[1].astype(jnp.int32))
    )

    bounds = [0] + [min(GROUP * k + 1, strips) for k in range(1, groups)] + [strips]

    def piece(number):
        if number == groups:
            return 0, LANES
        if number == groups + 1:
            return LANES + cols, LANES
        return LANES + bounds[number] * LANES, (bounds[number + 1] - bounds[number]) * LANES

    def lat_copy(side, number):
        start, width = piece(number)
        source_start, other = start, lon
        if number == groups:
            source_start, start, other = LANES, LANES + cols, west
        if number == groups + 1:
            source_start, start, other = cols, 0, east
        index = number
        if number == groups:
            index = groups + 1
        if number == groups + 1:
            index = groups
        target_row = HALO + rows if side == 0 else 0
        return pltpu.make_async_remote_copy(
            src_ref=zbuf.at[pl.ds(HALO + edge_rows[side], HALO), pl.ds(source_start, width)],
            dst_ref=zbuf.at[pl.ds(target_row, HALO), pl.ds(start, width)],
            send_sem=send_sem.at[side, number],
            recv_sem=recv_sem.at[1 - side, index],
            device_id=(neighbour[side], other),
            device_id_type=MESH,
        )

    def rim_copy(side):
        source_start, start, other = ((LANES, LANES + cols, west), (cols, 0, east))[side]
        return pltpu.make_async_remote_copy(
            src_ref=zbuf.at[pl.ds(HALO, rows), pl.ds(source_start, LANES)],
            dst_ref=zbuf.at[pl.ds(HALO, rows), pl.ds(start, LANES)],
            send_sem=rim_send.at[side],
            recv_sem=rim_recv.at[side],
            device_id=(lat, other),
            device_id_type=MESH,
        )

    order = [groups + 1] + list(range(groups)) + [groups]
    for side in range(2):
        loads[side].wait()

        @pl.when(exists[side])
        def _():
            for number in order:
                lat_copy(side, number).start()

    loads[2].wait()
    for side in range(2):
        rim_copy(side).start()

    def column_of(group):
        return pl.multiple_of(group * (GROUP * LANES), LANES)

    def rotate(row, octaves, group):
        column = column_of(group)
        z = [zbuf[pl.ds(row, SUB), pl.ds(column + k * LANES, LANES)] for k in range(GROUP + 2)]
        found = []
        for octave in octaves:
            stride = 2**octave
            scaled = [v * (1.0 / stride) for v in z] if octave else z
            ahead = [pltpu.roll(v, LANES - stride, 1) for v in scaled[1:]]
            if 2 * stride == LANES:
                behind = [pltpu.roll(scaled[0], stride, 1)] + ahead[:-1]
            else:
                behind = [pltpu.roll(v, stride, 1) for v in scaled[:-1]]
            found.append((octave, scaled, ahead, behind))
        return found

    def store(row, found, group, with_centre):
        centre = [None] * GROUP
        for octave, scaled, ahead, behind in found:
            stride = 2**octave
            store_row = pl.multiple_of(row - HALO + row_pad(stride), SUB)
            for k in range(GROUP):
                plus = jnp.where(lane < LANES - stride, ahead[k], ahead[k + 1])
                minus = jnp.where(lane >= stride, behind[k + 1], behind[k])
                strip = group * GROUP + k
                lags[octave][0, strip, pl.ds(store_row, SUB), :] = scaled[k + 1] + plus
                lags[octave][1, strip, pl.ds(store_row, SUB), :] = scaled[k + 1] + minus
                if with_centre:
                    term = plus - minus
                    centre[k] = term if centre[k] is None else centre[k] + term
        if with_centre:
            for k in range(GROUP):
                wsum[group * GROUP + k, pl.ds(pl.multiple_of(row - HALO, SUB), SUB), :] = (
                    centre[k] + centre[k]
                )

    def shade(row, group):
        coef = coef_ref[pl.ds(row, SUB), :]
        for k in range(GROUP):
            strip = group * GROUP + k
            down = up = None
            for octave in range(SCALES):
                stride = 2**octave
                lag = lags[octave]
                north = pl.ds(row + (row_pad(stride) - stride), SUB)
                south = pl.ds(row + (row_pad(stride) + stride), SUB)
                a = lag[0, strip, south, :] - lag[1, strip, north, :]
                b = lag[0, strip, north, :] - lag[1, strip, south, :]
                down = a if down is None else down + a
                up = b if up is None else up + b
            grad_east = (wsum[strip, pl.ds(row, SUB), :] + (down + up)) * coef
            grad_north = (up - down) * (1.0 / (8.0 * SCALES))
            squared = grad_east * grad_east + grad_north * grad_north
            inverse = lax.rsqrt(1.0 + squared)
            sine = squared * lax.rsqrt(jnp.maximum(squared, 1e-37)) * inverse
            ratio = jnp.full_like(inverse, ANGLE[-1])
            for term in ANGLE[-2::-1]:
                ratio = ratio * inverse + term
            facing_east = -grad_east * inverse
            facing_north = -grad_north * inverse
            shading = jnp.maximum(0.5 * (facing_north - facing_east) + LIGHT_UP * inverse, 0.0)
            place = (pl.ds(row, SUB), pl.ds(column_of(group) + k * LANES, LANES))
            slope_ref[place] = sine * ratio
            facing_ref[(0,) + place] = facing_east
            facing_ref[(1,) + place] = facing_north
            shade_ref[place] = shading

    near = 1 - lax.rem(lat, 2)
    far = 1 - near
    near_top = near == 0
    far_exists = jnp.where(near_top, exists[1], exists[0])

    def row_at(step):
        return pl.multiple_of(jnp.where(near_top, step * SUB, rows - SUB - step * SUB), SUB)

    def halo_row(side):
        return pl.multiple_of(jnp.where(side == 0, 0, HALO + rows), SUB)

    def wait_piece(side, number):
        start, width = piece(number)
        here = zbuf.at[pl.ds(halo_row(side), HALO), pl.ds(start, width)]
        pltpu.make_async_remote_copy(
            src_ref=here,
            dst_ref=here,
            send_sem=send_sem.at[0, number],
            recv_sem=recv_sem.at[side, number],
            device_id=(lat, east),
            device_id_type=MESH,
        ).wait_recv()

    def widen_halo(side, group):
        for distance in range(0, HALO, SUB):
            row = pl.multiple_of(
                jnp.where(side == 0, HALO - SUB - distance, HALO + rows + distance), SUB
            )
            octaves = [k for k in range(SCALES) if row_pad(2**k) > distance]
            store(row, rotate(row, octaves, group), group, False)

    ahead_steps = HALO // SUB + 1
    steps = rows // SUB

    def inner(index, carry):
        group = lax.rem(index + 1, groups)

        @pl.when(index == max(groups - 2, 0))
        def _():
            for side in range(2):
                rim_copy(side).wait_recv()

        def alone(step, carry):
            row = row_at(step) + HALO
            store(row, rotate(row, range(SCALES), group), group, True)
            return carry

        lax.fori_loop(0, ahead_steps, alone, 0)

        @pl.when(index == 0)
        def _():
            for number in order:
                wait_piece(near, number)

        widen_halo(near, group)

        def both(step, carry):
            row = row_at(step + ahead_steps) + HALO
            found = rotate(row, range(SCALES), group)
            shade(row_at(step), group)
            store(row, found, group, True)
            return carry

        lax.fori_loop(0, steps - ahead_steps, both, 0)
        return carry

    lax.fori_loop(0, groups, inner, 0)

    for pole in range(2):

        @pl.when(jnp.logical_and(jnp.logical_not(far_exists), far == pole))
        def _():
            first = HALO if pole == 0 else HALO + rows - SUB
            pick = 0 if pole == 0 else SUB - 1
            fill = 0 if pole == 0 else HALO + rows

            def repeat(strip, carry):
                column = pl.ds(pl.multiple_of(strip * LANES, LANES), LANES)
                edge = zbuf[pl.ds(first, SUB), column][pick : pick + 1]
                block = jnp.broadcast_to(edge, (SUB, LANES))
                for k in range(HALO // SUB):
                    zbuf[pl.ds(fill + k * SUB, SUB), column] = block
                return carry

            lax.fori_loop(0, strips + 2, repeat, 0)

    def last(group, carry):
        for k in range(groups):

            @pl.when(jnp.logical_and(far_exists, group == k))
            def _():
                wait_piece(far, k)
                if k == 0:
                    wait_piece(far, groups)
                if k == groups - 1:
                    wait_piece(far, groups + 1)

        widen_halo(far, group)

        def finish(step, carry):
            shade(row_at(step + steps - ahead_steps), group)
            return carry

        lax.fori_loop(0, ahead_steps, finish, 0)
        return carry

    lax.fori_loop(0, groups, last, 0)

    for side in range(2):
        rim_copy(side).wait_send()

        @pl.when(exists[side])
        def _():
            for number in order:
                lat_copy(side, number).wait_send()


def local(elevation):
    rows, cols = elevation.shape
    strips = cols // LANES
    groups = strips // GROUP
    return tuple(
        pl.pallas_call(
            functools.partial(kernel, rows, cols),
            out_shape=(
                pltpu.VMEM((rows, cols), jnp.float32),
                pltpu.VMEM((2, rows, cols), jnp.float32),
                pltpu.VMEM((rows, cols), jnp.float32),
            ),
            in_specs=[
                pl.BlockSpec(memory_space=pl.ANY),
            ],
            out_specs=tuple([pl.BlockSpec(memory_space=pltpu.VMEM)] * 3),
            scratch_shapes=[
                pltpu.VMEM((2, strips, rows + 2 * row_pad(2**k), LANES), jnp.float32)
                for k in range(SCALES)
            ]
            + [
                pltpu.VMEM((rows + 2 * HALO, cols + 2 * LANES), jnp.float32),
                pltpu.VMEM((strips, rows, LANES), jnp.float32),
                pltpu.VMEM((rows, LANES), jnp.float32),
                pltpu.SemaphoreType.DMA((3,)),
                pltpu.SemaphoreType.DMA((2, groups + 2)),
                pltpu.SemaphoreType.DMA((2, groups + 2)),
                pltpu.SemaphoreType.DMA((2,)),
                pltpu.SemaphoreType.DMA((2,)),
            ],
            compiler_params=pltpu.CompilerParams(
                collective_id=0, has_side_effects=True, vmem_limit_bytes=52 * 2**20
            ),
        )(elevation)
    )


def solution(mesh):
    in_specs = (P("lat", "lon"),)
    out_specs = (P("lat", "lon"), P(None, "lat", "lon"), P("lat", "lon"))
    return jax.shard_map(local, mesh=mesh, in_specs=in_specs, out_specs=out_specs, check_vma=False)
```
